32 devices in a mesh: cp: 8 (over z, x), tp: 4 (over y, core).
Axes of the slice: x: 2, y: 2, z: 4, core: 2. Of those that a mesh axis runs over, the one named last changes fastest.
Arguments:
- queries: bfloat16 [1024, 8192], P('cp', 'tp'), may hold values from -6 to 6
- keys: bfloat16 [1024, 1024], P('cp', 'tp'), may hold values from -6 to 6
- values: bfloat16 [1024, 1024], P('cp', 'tp'), may hold values from -6 to 6
- doc_blocks: int32 [4], replicated, may hold values from 1 to 4, 8 in all
- block_order: int32 [8], replicated, may hold values from 0 to 7, each once
- out_weight: bfloat16 [8192, 4096], P('tp'), may hold values from -0.5 to 0.5
Outputs:
- layer_out: bfloat16 [1024, 4096], P(('cp', 'tp'))
The draws below stay inside these ranges and needn't reach their ends.
Inputs may be any that keep to these rules, and one draw needn't show every extreme that they name: Array block i (rows i * 128 to i * 128 + 127) holds sequence block block_order[i]; every block number appears once. `doc_blocks`: they sum to 8; the longest document has exactly 4 blocks.
All inputs are finite; a program needn't handle non-finite values.
Results may differ from the reference program's by a relative error of at most 0.013.
Values may be sent and summed in bfloat16 or wider, within the bound.
A program may use at most 128 MiB of HBM per device.

```python
import math
import jax
import jax.numpy as jnp
import numpy as np
from jax import lax

QUERY_HEADS = 64
KEY_VALUE_HEADS = 8
HEAD_SIZE = 128
WIN = 4096
BLOCK_TOKENS = 128
NDOC = 4
GROUP_HEADS = 8
PACK_TOKENS = 1024
NBLK = 8
MOSTB = 4


def draw_keys(key, part):
    picked_rows = jax.random.truncated_normal(jax.random.fold_in(key, 13), -4.0, 4.0, (PACK_TOKENS, KEY_VALUE_HEADS * HEAD_SIZE), jnp.float32)
    return picked_rows.astype(jnp.bfloat16)


def draw_queries(key, part):
    picked_rows = jax.random.truncated_normal(jax.random.fold_in(key, 14), -4.0, 4.0, (PACK_TOKENS, QUERY_HEADS * HEAD_SIZE), jnp.float32)
    return picked_rows.astype(jnp.bfloat16)


def level_of(own_key, dims, pieces, smallest, top_value):
    factor_of, own = 1.0, jax.random.fold_in(own_key, 6)
    for dim, blocks in pieces:
        heights = jnp.exp(jax.random.uniform(jax.random.fold_in(own, dim), (blocks,), jnp.float32, smallest / len(pieces), top_value / len(pieces)))
        factor_of = factor_of * jnp.repeat(heights, dims[dim] // blocks).reshape([-1 if axis == dim else 1 for axis in range(len(dims))])
    return factor_of


def split_up(count, total, most, slope):
    weights = [(1 << 20) // math.isqrt(standing ** slope) + 1 for standing in range(2, count + 1)]
    surplus, counts = total - most - (count - 1), [1] * (count - 1)
    while surplus > 0:
        movable = [i for i in range(count - 1) if counts[i] < most]
        mass, remaining = sum([weights[i] for i in movable]), surplus
        for i in movable:
            extra = min(most - counts[i], max(1, remaining * weights[i] // mass), surplus)
            counts[i] = counts[i] + extra
            surplus = surplus - extra
    return np.array([most] + counts)


def uneven_parts(stream_key, amount, total, reach, lean):
    if amount == 2:
        one = jax.random.randint(stream_key, (), max(1, total - reach), min(reach, total - 1) + 1)
        return jnp.stack([one, total - one])
    tallies = jnp.asarray(split_up(amount, total, reach, lean), jnp.int32)
    pairs = (amount - 1) // 2
    giver, sink = tallies[1:1 + 2 * pairs:2], tallies[2:2 + 2 * pairs:2]
    margin = jnp.minimum(giver - 1, reach - sink)
    passed = jax.random.randint(jax.random.fold_in(stream_key, 1), (pairs,), 0, 1 << 20) % (margin + 1)
    tallies = tallies.at[1:1 + 2 * pairs:2].set(giver - passed).at[2:2 + 2 * pairs:2].set(sink + passed)
    return tallies[jax.random.permutation(jax.random.fold_in(stream_key, 2), amount)]


def scatter_about(rng, shape, scale, bound, shards=(), kind=jnp.bfloat16):
    level = level_of(rng, shape, shards, -0.22, 0.18) if shards else 1.0
    values = jax.random.normal(rng, shape, jnp.float32) * scale * level
    return jnp.minimum(jnp.maximum(values, -bound), bound).astype(kind)


def setup_inputs(seed: int = 0) -> dict:
    arg_keys = jax.random.split(jax.random.key(seed), 7)
    queries = draw_queries(jax.random.fold_in(arg_keys[6], 71), 0)
    keys = draw_keys(jax.random.fold_in(arg_keys[6], 71), 0)
    values = scatter_about(arg_keys[2], (PACK_TOKENS, KEY_VALUE_HEADS * HEAD_SIZE), 1.0, 6.0, ((0, 8), (1, 4)))
    doc_blocks = uneven_parts(arg_keys[3], NDOC, NBLK, MOSTB, 2).astype(jnp.int32)
    block_order = jax.random.permutation(arg_keys[4], NBLK).astype(jnp.int32)
    out_weight = scatter_about(arg_keys[5], (QUERY_HEADS * HEAD_SIZE, WIN), HEAD_SIZE ** -0.5, 0.5, ((0, 4),))
    return dict(queries=queries, keys=keys, values=values, doc_blocks=doc_blocks, block_order=block_order, out_weight=out_weight)


document_masked_score = -1.0e30


def reference(queries, keys, values, doc_blocks, block_order, out_weight):
    token_blocks = PACK_TOKENS // BLOCK_TOKENS
    block_ids = jnp.arange(token_blocks, dtype=jnp.int32)
    inverse_order = jnp.zeros((token_blocks,), jnp.int32).at[block_order].set(block_ids)
    sequence_queries = queries.reshape(token_blocks, BLOCK_TOKENS, KEY_VALUE_HEADS, GROUP_HEADS, HEAD_SIZE)[inverse_order]
    sequence_keys = keys.reshape(token_blocks, BLOCK_TOKENS, KEY_VALUE_HEADS, HEAD_SIZE)[inverse_order]
    sequence_values = values.reshape(token_blocks, BLOCK_TOKENS, KEY_VALUE_HEADS, HEAD_SIZE)[inverse_order]
    doc_ends = jnp.cumsum(doc_blocks).astype(jnp.int32)
    doc_of = jnp.sum((block_ids[:, None] >= doc_ends[None, :]).astype(jnp.int32), axis=1)
    doc_first = (doc_ends - doc_blocks).astype(jnp.int32)[doc_of]
    inner = jnp.arange(BLOCK_TOKENS, dtype=jnp.int32)

    def one_block(seq_block):
        query_rows = sequence_queries[seq_block].astype(jnp.float32)

        def add_tile(key_block, online):
            running_max, weight_sum, weighted = online
            key_rows = sequence_keys[key_block].astype(jnp.float32)
            value_rows = sequence_values[key_block].astype(jnp.float32)
            scores = jnp.einsum('qhgd,khd->hgqk', query_rows, key_rows) * (HEAD_SIZE ** -0.5)
            allowed = (key_block * BLOCK_TOKENS + inner[None, :]) <= (seq_block * BLOCK_TOKENS + inner[:, None])
            scores = jnp.where(allowed, scores, document_masked_score)
            new_max = jnp.maximum(running_max, jnp.max(scores, axis=-1))
            weights = jnp.where(allowed, jnp.exp(scores - new_max[..., None]), 0.0)
            factor = jnp.exp(running_max - new_max)
            weight_sum = weight_sum * factor + jnp.sum(weights, axis=-1)
            rounded = lax.optimization_barrier(weights.astype(jnp.bfloat16)).astype(jnp.float32)
            weighted = weighted * factor[..., None] + jnp.einsum('hgqk,khd->hgqd', rounded, value_rows)
            return new_max, weight_sum, weighted

        starting_state = (jnp.full((KEY_VALUE_HEADS, GROUP_HEADS, BLOCK_TOKENS), document_masked_score, jnp.float32),
                   jnp.zeros((KEY_VALUE_HEADS, GROUP_HEADS, BLOCK_TOKENS), jnp.float32),
                   jnp.zeros((KEY_VALUE_HEADS, GROUP_HEADS, BLOCK_TOKENS, HEAD_SIZE), jnp.float32))
        running_max, weight_sum, weighted = lax.fori_loop(doc_first[seq_block], seq_block + 1, add_tile, starting_state)
        result = weighted / weight_sum[..., None]
        return jnp.transpose(result, (2, 0, 1, 3)).reshape(BLOCK_TOKENS, QUERY_HEADS * HEAD_SIZE).astype(jnp.bfloat16)

    attended_seq = lax.map(one_block, block_ids)
    attended = attended_seq[block_order].reshape(PACK_TOKENS, QUERY_HEADS * HEAD_SIZE)
    return jnp.dot(attended, out_weight, preferred_element_type=jnp.float32).astype(jnp.bfloat16)
```

```python
import functools

import jax
import jax.numpy as jnp
from jax import lax
from jax.experimental import pallas as pl
from jax.experimental.pallas import tpu as pltpu
from jax.sharding import PartitionSpec as P

HEAD_SIZE = 128
BLOCK_TOKENS = 128
MASKED = -1e30
LOG2E = 1.4426950408889634
MESH = pl.DeviceIdType.MESH


def kernel(
    nc, ndoc, chunks,
    q_hbm, k_hbm, v_hbm, doc_hbm, ord_hbm, w_hbm, o_hbm,
    w_v, q_v, kv, m_s, acc, att, p_v, r1, s2, r2, o_v,
    kv_sem, q_sem, w_sem, dn_send, z_send, x_send, ag_recv, c_send, c_recv, y_send, y_recv, o_sem, doc_ref, ord_ref, s_sem,
):
    D = HEAD_SIZE
    me = lax.axis_index("cp")
    tp = lax.axis_index("tp")
    core = lax.rem(tp, 2)
    yy = lax.div(tp, 2)
    sib = yy * 2 + (1 - core)
    ypeer = (1 - yy) * 2 + core
    cz = nc // 2
    z = lax.div(me, 2)
    x = lax.rem(me, 2)
    heads_kv = kv.shape[1]
    group = q_v.shape[1] // (heads_kv * D)
    width = w_v.shape[2]

    local = []
    for h in range(heads_kv):
        for i, src in enumerate((k_hbm, v_hbm)):
            local.append(pltpu.make_async_copy(
                src.at[:, pl.ds(h * D, D)], kv.at[me, h, i], kv_sem.at[2 * h + i]))
    for c in local:
        c.start()
    q_copy = pltpu.make_async_copy(q_hbm, q_v, q_sem)
    q_copy.start()

    def w_copy(c):
        return pltpu.make_async_copy(
            w_hbm.at[:, pl.ds(c * width, width)], w_v.at[c], w_sem.at[c])

    sc = [pltpu.make_async_copy(doc_hbm, doc_ref, s_sem.at[0]), pltpu.make_async_copy(ord_hbm, ord_ref, s_sem.at[1])]
    for c in sc: c.start()
    barrier = pltpu.get_barrier_semaphore()

    has_up, has_dn = z + 1 < cz, z > 0
    nb = z * 2 + (1 - x)

    def greet(where):
        pl.semaphore_signal(barrier, inc=1, device_id=where, device_id_type=MESH)

    pl.when(has_up)(lambda: greet({"cp": me + 2}))
    pl.when(has_dn)(lambda: greet({"cp": me - 2}))
    greet({"cp": nb})
    greet({"tp": sib})
    greet({"tp": ypeer})
    pl.semaphore_wait(barrier, 3 + jnp.where(has_up, 1, 0) + jnp.where(has_dn, 1, 0))

    def hop(b, h, dst, sem):
        return pltpu.make_async_remote_copy(
            src_ref=kv.at[b, h], dst_ref=kv.at[b, h],
            send_sem=sem, recv_sem=ag_recv.at[b, h],
            device_id={"cp": dst}, device_id_type=MESH)

    def own_up(h):
        return hop(me, h, me + 2, z_send.at[me, h])

    def own_dn(h):
        return hop(me, h, me - 2, dn_send.at[h])

    def over_x(b, h):
        return hop(b, h, nb, x_send.at[b, h])

    def over_z(b, h, dst):
        return hop(b, h, dst, z_send.at[b, h])

    for h in range(heads_kv):
        local[2 * h].wait()
        local[2 * h + 1].wait()
        pl.when(has_up)(lambda: own_up(h).start())
        pl.when(has_dn)(lambda: own_dn(h).start())
        over_x(me, h).start()

    early = 2
    for c in range(early):
        w_copy(c).start()

    left, right = z, cz - 1 - z
    near = jnp.where(left < right, left, right)
    far_side = jnp.where(left < right, 1, -1)

    def nearest(j):
        both = j <= 2 * near
        side = jnp.where(both, 2 * lax.rem(j, 2) - 1, far_side)
        zz = z + side * jnp.where(both, lax.div(j + 1, 2), j - near)
        return zz * 2 + x, zz * 2 + (1 - x), z - side

    for c in sc: c.wait()
    ends = []
    total = 0
    for d in range(ndoc):
        total = total + doc_ref[d]
        ends.append(total)

    def place(b):
        s = ord_ref[b]
        doc = jnp.int32(0)
        for e in ends:
            doc = doc + jnp.where(s >= e, 1, 0).astype(jnp.int32)
        return s, doc

    s0, d0 = place(me)

    def bias_of(b):
        s, doc = place(b)
        return jnp.where((doc == d0) & (s < s0), 0.0, MASKED).astype(jnp.float32)

    scale = HEAD_SIZE ** -0.5 * LOG2E
    tile = 2 * BLOCK_TOKENS
    col = lax.broadcasted_iota(jnp.int32, (tile, tile), 1)
    row = lax.broadcasted_iota(jnp.int32, (tile, tile), 0)
    col1 = lax.broadcasted_iota(jnp.int32, (1, tile), 1)
    ones = jnp.ones((tile, D), jnp.bfloat16)

    def step(b0, b1, bias, first, heads):
        for h in heads:
            k2 = jnp.concatenate([kv[b0, h, 0], kv[b1, h, 0]], axis=0)
            v2 = jnp.concatenate([kv[b0, h, 1], kv[b1, h, 1]], axis=0)
            v2 = jnp.concatenate([v2, ones], axis=1)
            for t in range(group // 2):
                hq = h * group + 2 * t
                q2 = jnp.concatenate(
                    [q_v[:, hq * D:(hq + 1) * D], q_v[:, (hq + 1) * D:(hq + 2) * D]], axis=0)
                s = lax.dot_general(
                    q2, k2, (((1,), (1,)), ((), ())), preferred_element_type=jnp.float32)
                s = s * scale + bias
                top = jnp.max(s, axis=1, keepdims=True)
                rows = pl.ds(hq * BLOCK_TOKENS, tile)
                if first:
                    m_new = top
                else:
                    m_old = m_s[rows, 0:1]
                    m_new = jnp.maximum(m_old, top)
                p = jnp.exp2(s - m_new).astype(jnp.bfloat16)
                pv = jnp.dot(p, v2, preferred_element_type=jnp.float32)
                if first:
                    acc[rows, :] = pv
                else:
                    acc[rows, :] = acc[rows, :] * jnp.exp2(m_old - m_new) + pv
                m_s[rows, :] = jnp.broadcast_to(m_new, (tile, D))

    inside = row - jnp.where(row >= BLOCK_TOKENS, BLOCK_TOKENS, 0)
    bias0 = jnp.where(
        col >= BLOCK_TOKENS, bias_of(nb), jnp.where(col <= inside, 0.0, MASKED))

    def pass_on(j, h):
        b, _, nxt = nearest(j)
        over_x(b, h).wait_recv()
        pl.when((nxt >= 0) & (nxt < cz))(lambda: over_z(b, h, nxt * 2 + x).start())
        over_x(b, h).start()
        c = early + (j - 1) * heads_kv + h
        pl.when(c < chunks)(lambda: w_copy(c).start())

    def attend(j, h):
        b0, b1, _ = nearest(j)
        bias = jnp.where(col1 >= BLOCK_TOKENS, bias_of(b1), bias_of(b0))
        over_x(b1, h).wait_recv()
        step(b0, b1, bias, False, (h,))

    q_copy.wait()
    for h in range(heads_kv):
        pass_on(1, h)
        over_x(nb, h).wait_recv()
        step(me, nb, bias0, True, (h,))

    @pl.loop(2, cz)
    def _(j):
        for h in range(heads_kv):
            pass_on(j, h)
            attend(j - 1, h)

    for c in range(min(chunks, early + (cz - 1) * heads_kv), chunks):
        w_copy(c).start()
    for h in range(heads_kv):
        attend(cz - 1, h)

    for hq in range(heads_kv * group):
        rows = pl.ds(hq * BLOCK_TOKENS, BLOCK_TOKENS)
        att[:, hq * D:(hq + 1) * D] = (acc[rows, :D] / acc[rows, D:]).astype(jnp.bfloat16)

    strip = BLOCK_TOKENS // 4

    def c_copy(c):
        return pltpu.make_async_remote_copy(
            src_ref=p_v.at[c, 1 - core], dst_ref=r1.at[c],
            send_sem=c_send.at[c], recv_sem=c_recv.at[c],
            device_id={"tp": sib}, device_id_type=MESH)

    def y_copy(c):
        return pltpu.make_async_remote_copy(
            src_ref=s2.at[c], dst_ref=r2.at[c],
            send_sem=y_send.at[c], recv_sem=y_recv.at[c],
            device_id={"tp": ypeer}, device_id_type=MESH)

    def o_copy(c):
        return pltpu.make_async_copy(
            o_v.at[c], o_hbm.at[:, pl.ds(c * width, width)], o_sem.at[c])

    def stage1(c):
        w_copy(c).wait()
        part = jnp.dot(att[...], w_v[c], preferred_element_type=jnp.float32)
        part = part.astype(jnp.bfloat16)
        for t in range(4):
            p_v[c, t % 2, t // 2] = part[t * strip:(t + 1) * strip]
        c_copy(c).start()

    def stage2(c):
        c_copy(c).wait_recv()
        s2[c] = (p_v[c, core, 1 - yy].astype(jnp.float32)
                 + r1[c, 1 - yy].astype(jnp.float32)).astype(jnp.bfloat16)
        y_copy(c).start()

    def stage3(c):
        y_copy(c).wait_recv()
        o_v[c] = (p_v[c, core, yy].astype(jnp.float32) + r1[c, yy].astype(jnp.float32)
                  + r2[c].astype(jnp.float32)).astype(jnp.bfloat16)
        o_copy(c).start()

    lag2, lag3 = 1, 5
    for i in range(chunks + lag3):
        if i < chunks:
            stage1(i)
        if 0 <= i - lag2 < chunks:
            stage2(i - lag2)
        if 0 <= i - lag3 < chunks:
            stage3(i - lag3)

    for h in range(heads_kv):
        pl.when(has_up)(lambda: own_up(h).wait_send())
        pl.when(has_dn)(lambda: own_dn(h).wait_send())
        over_x(me, h).wait_send()

    @pl.loop(1, cz)
    def _(j):
        b, _, nxt = nearest(j)
        for h in range(heads_kv):
            pl.when((nxt >= 0) & (nxt < cz))(lambda: over_z(b, h, nxt * 2 + x).wait_send())
            over_x(b, h).wait_send()

    for c in range(chunks):
        c_copy(c).wait_send()
        y_copy(c).wait_send()
        o_copy(c).wait()


def local_fn(nc, queries, keys, values, doc_blocks, block_order, out_weight):
    rows, qcols = queries.shape
    depth, cols = out_weight.shape
    heads_kv = keys.shape[1] // HEAD_SIZE
    chunks = 8
    width = cols // chunks
    strip = rows // 4
    bf, f32 = jnp.bfloat16, jnp.float32
    dma = pltpu.SemaphoreType.DMA
    hbm = pl.BlockSpec(memory_space=pltpu.HBM)
    anyspec = pl.BlockSpec(memory_space=pl.ANY)
    smem = pl.BlockSpec(memory_space=pltpu.SMEM)
    return pl.pallas_call(
        functools.partial(kernel, nc, doc_blocks.shape[0], chunks),
        out_shape=jax.ShapeDtypeStruct((strip, cols), bf),
        in_specs=[hbm, hbm, hbm, hbm, hbm, hbm],
        out_specs=anyspec,
        scratch_shapes=[
            pltpu.VMEM((chunks, depth, width), bf),
            pltpu.VMEM((rows, qcols), bf),
            pltpu.VMEM((nc, heads_kv, 2, BLOCK_TOKENS, HEAD_SIZE), bf),
            pltpu.VMEM((qcols, HEAD_SIZE), f32),
            pltpu.VMEM((qcols, 2 * HEAD_SIZE), f32),
            pltpu.VMEM((rows, qcols), bf),
            pltpu.VMEM((chunks, 2, 2, strip, width), bf),
            pltpu.VMEM((chunks, 2, strip, width), bf),
            pltpu.VMEM((chunks, strip, width), bf),
            pltpu.VMEM((chunks, strip, width), bf),
            pltpu.VMEM((chunks, strip, width), bf),
            dma((2 * heads_kv,)), dma, dma((chunks,)),
            dma((heads_kv,)), dma((nc, heads_kv)), dma((nc, heads_kv)), dma((nc, heads_kv)),
            dma((chunks,)), dma((chunks,)), dma((chunks,)), dma((chunks,)), dma((chunks,)), pltpu.SMEM(doc_blocks.shape, jnp.int32), pltpu.SMEM(block_order.shape, jnp.int32), dma((2,)),
        ],
        compiler_params=pltpu.CompilerParams(
            collective_id=0, has_side_effects=True, vmem_limit_bytes=40 * 2**20),
    )(*[pltpu.with_memory_space_constraint(a, pltpu.HBM) for a in (queries, keys, values, doc_blocks, block_order, out_weight)])


def solution(mesh):
    placed = (P("cp", "tp"), P("cp", "tp"), P("cp", "tp"), P(), P(), P("tp", None))
    assert mesh.shape["tp"] == 4
    return jax.shard_map(
        functools.partial(local_fn, mesh.shape["cp"]),
        mesh=mesh, in_specs=placed, out_specs=P(("cp", "tp"), None), check_vma=False,
    )
```

```python
import functools

import jax
import jax.numpy as jnp
from jax import lax
from jax.experimental import pallas as pl
from jax.experimental.pallas import tpu as pltpu
from jax.sharding import PartitionSpec as P

HEAD_SIZE = 128
BLOCK_TOKENS = 128
MASKED = -1e30
LOG2E = 1.4426950408889634
MESH = pl.DeviceIdType.MESH
GROUP_BLOCKS = 4
UNROLL = 4


def each(lo, hi, body):
    if hi - lo <= UNROLL:
        for j in range(lo, hi):
            body(j)
    else:
        pl.loop(lo, hi)(body)


def kernel(nc, ndoc, chunks, heads_kv, q_hbm, k_hbm, v_hbm, doc_hbm, ord_hbm, w_hbm, o_ref, *scratch):
    D = HEAD_SIZE
    (doc_ref, ord_ref, w_v, q_v, att, p_v, r1, s2, r2, m_s, acc,
     s_sem, kv_sem, q_sem, w_sem, up_send, dn_send, x_send, ag_recv,
     c_send, c_recv, y_send, y_recv) = scratch[:23]
    kv = scratch[23:]
    me = lax.axis_index("cp")
    tp = lax.axis_index("tp")
    core = lax.rem(tp, 2)
    yy = lax.div(tp, 2)
    sib = yy * 2 + (1 - core)
    ypeer = (1 - yy) * 2 + core
    cz = nc // 2
    z = lax.div(me, 2)
    x = lax.rem(me, 2)
    nb = z * 2 + (1 - x)
    group = q_v.shape[1] // (heads_kv * D)
    width = w_v.shape[2]
    span = nc // 2

    def buf(h, c):
        return kv[2 * h + c]

    pieces = [(h, c) for c in (1, 0) for h in range(heads_kv)]
    local = {}
    for h, c in pieces:
        local[h, c] = pltpu.make_async_copy(
            (k_hbm, v_hbm)[c].at[:, pl.ds(h * D, D)], buf(h, c).at[me], kv_sem.at[h, c])
    for h, c in pieces:
        local[h, c].start()
    small = [pltpu.make_async_copy(doc_hbm, doc_ref, s_sem.at[0]),
             pltpu.make_async_copy(ord_hbm, ord_ref, s_sem.at[1])]
    for s in small:
        s.start()
    q_copy = pltpu.make_async_copy(q_hbm, q_v, q_sem)
    q_copy.start()

    def w_copy(c):
        return pltpu.make_async_copy(
            w_hbm.at[:, pl.ds(c * width, width)], w_v.at[c], w_sem.at[c])

    barrier = pltpu.get_barrier_semaphore()
    has_up, has_dn = z + 1 < cz, z > 0

    def greet(where):
        pl.semaphore_signal(barrier, inc=1, device_id=where, device_id_type=MESH)

    pl.when(has_up)(lambda: greet({"cp": me + 2}))
    pl.when(has_dn)(lambda: greet({"cp": me - 2}))
    greet({"cp": nb})
    greet({"tp": sib})
    greet({"tp": ypeer})
    pl.semaphore_wait(barrier, 3 + jnp.where(has_up, 1, 0) + jnp.where(has_dn, 1, 0))

    def hop(b, h, c, dst, sem):
        return pltpu.make_async_remote_copy(
            src_ref=buf(h, c).at[b], dst_ref=buf(h, c).at[b],
            send_sem=sem.at[b, h, c], recv_sem=ag_recv.at[b, h, c],
            device_id={"cp": dst}, device_id_type=MESH)

    def over_x(b, h, c):
        return hop(b, h, c, nb, x_send)

    def along(b, h, c, side):
        if side > 0:
            return hop(b, h, c, me - 2, dn_send)
        return hop(b, h, c, me + 2, up_send)

    def within(level):
        return (level >= 0) & (level < cz)

    def is_end(level):
        return (level == 0) | (level == cz - 1)

    for h, c in pieces:
        local[h, c].wait()
        pl.when(has_up)(lambda: along(me, h, c, -1).start())
        pl.when(has_dn)(lambda: along(me, h, c, 1).start())
    for h, c in reversed(pieces):
        over_x(me, h, c).start()

    for c in range(chunks):
        w_copy(c).start()

    def column(d, h, c, side, act_z, act_x, wait):
        zb = z + side * d

        @pl.when(within(zb))
        def _():
            b = zb * 2 + x
            if wait:
                over_x(b, h, c).wait_recv()
            pl.when(within(z - side))(lambda: act_z(along(b, h, c, side)))
            if c == 0:
                pl.when(jnp.logical_not(is_end(zb)))(lambda: act_x(over_x(b, h, c)))
            else:
                act_x(over_x(b, h, c))

    def cross(d, h, side, act_z, wait):
        zb = z + side * d

        @pl.when(zb == (cz - 1 if side > 0 else 0))
        def _():
            b = zb * 2 + (1 - x)
            if wait:
                over_x(b, h, 0).wait_recv()
            pl.when(within(z - side))(lambda: act_z(along(b, h, 0, side)))

    def relay(d, act_z, act_x, wait):
        for i, (h, c) in enumerate(pieces):
            for side in (1, -1):
                column(d, h, c, side, act_z, act_x, wait)
            if i < heads_kv:
                for side in (1, -1):
                    cross(d - 1, i, side, act_z, wait)

    def start(copy):
        copy.start()

    def sent(copy):
        copy.wait_send()

    each(1, cz, lambda d: relay(d, start, start, True))

    for s in small:
        s.wait()
    ends = []
    total = 0
    for d in range(ndoc):
        total = total + doc_ref[d]
        ends.append(total)

    def doc_of(s):
        doc = jnp.int32(0)
        for e in ends:
            doc = doc + jnp.where(s >= e, 1, 0).astype(jnp.int32)
        return doc

    s0 = ord_ref[me]
    d0 = doc_of(s0)

    def earlier(k):
        want = s0 - k
        if nc <= 8:
            at = me
            for b in range(nc):
                at = jnp.where(ord_ref[b] == want, b, at)
        else:
            at = lax.fori_loop(
                0, nc, lambda b, at: jnp.where(ord_ref[b] == want, b, at), me)
        kept = (want >= 0) & (doc_of(want) == d0) & (k > 0)
        return at, jnp.where(kept, 0.0, MASKED).astype(jnp.float32)

    scale = HEAD_SIZE ** -0.5 * LOG2E
    tile = 2 * BLOCK_TOKENS
    col = lax.broadcasted_iota(jnp.int32, (tile, BLOCK_TOKENS), 1)
    row = lax.broadcasted_iota(jnp.int32, (tile, BLOCK_TOKENS), 0)
    inside = row - jnp.where(row >= BLOCK_TOKENS, BLOCK_TOKENS, 0)
    causal = jnp.where(col <= inside, 0.0, MASKED).astype(jnp.float32)
    ones = jnp.ones((GROUP_BLOCKS * BLOCK_TOKENS, D), jnp.bfloat16)

    def attend(h, places, first, last):
        k4 = jnp.concatenate([buf(h, 0)[b] for b, _ in places], axis=0)
        v4 = jnp.concatenate([buf(h, 1)[b] for b, _ in places], axis=0)
        v4 = jnp.concatenate([v4, ones[:v4.shape[0]]], axis=1)
        for t in range(group // 2):
            hq = h * group + 2 * t
            q2 = jnp.concatenate(
                [q_v[:, hq * D:(hq + 1) * D], q_v[:, (hq + 1) * D:(hq + 2) * D]], axis=0)
            s = lax.dot_general(
                q2, k4, (((1,), (1,)), ((), ())), preferred_element_type=jnp.float32)
            parts = [s[:, i * BLOCK_TOKENS:(i + 1) * BLOCK_TOKENS] * scale + bias
                     for i, (_, bias) in enumerate(places)]
            top = parts[0]
            for part in parts[1:]:
                top = jnp.maximum(top, part)
            top = jnp.max(top, axis=1, keepdims=True)
            rows = pl.ds(hq * BLOCK_TOKENS, tile)
            if not first:
                old = m_s[rows, 0:1]
                top = jnp.maximum(old, top)
            p = jnp.concatenate(
                [jnp.exp2(part - top).astype(jnp.bfloat16) for part in parts], axis=1)
            pv = jnp.dot(p, v4, preferred_element_type=jnp.float32)
            if not first:
                pv = acc[rows, :] * jnp.exp2(old - top) + pv
            if last:
                out = (pv[:, :D] / pv[:, D:]).astype(jnp.bfloat16)
                att[:, hq * D:(hq + 1) * D] = out[:BLOCK_TOKENS]
                att[:, (hq + 1) * D:(hq + 2) * D] = out[BLOCK_TOKENS:]
            else:
                acc[rows, :] = pv
                m_s[rows, :] = jnp.broadcast_to(top, (tile, D))

    def final_waits(h):
        def level(zb):
            b = zb * 2 + (1 - x)
            over_x(b, h, 1).wait_recv()
            if isinstance(zb, int):
                if 0 < zb < cz - 1:
                    over_x(b, h, 0).wait_recv()
            else:
                pl.when(jnp.logical_not(is_end(zb)))(lambda: over_x(b, h, 0).wait_recv())
        each(0, cz, level)
        for side in (1, -1):
            cross(cz - 1, h, side, start, True)

    near = min(GROUP_BLOCKS, span)
    spots = [(me, causal)] + [earlier(k) for k in range(1, near)]
    q_copy.wait()
    for h in range(heads_kv):
        final_waits(h)
        attend(h, spots, True, span <= near)
        if span > near:
            assert span % near == 0

            @pl.loop(1, span // near - 1)
            def _(g):
                attend(h, [earlier(g * near + k) for k in range(near)], False, False)

            attend(h, [earlier(span - near + k) for k in range(near)], False, True)

    strip = BLOCK_TOKENS // 4

    def c_copy(c):
        return pltpu.make_async_remote_copy(
            src_ref=p_v.at[c, 1 - core], dst_ref=r1.at[c],
            send_sem=c_send.at[c], recv_sem=c_recv.at[c],
            device_id={"tp": sib}, device_id_type=MESH)

    def y_copy(c):
        return pltpu.make_async_remote_copy(
            src_ref=s2.at[c], dst_ref=r2.at[c],
            send_sem=y_send.at[c], recv_sem=y_recv.at[c],
            device_id={"tp": ypeer}, device_id_type=MESH)

    def stage1(c):
        w_copy(c).wait()
        part = jnp.dot(att[...], w_v[c], preferred_element_type=jnp.float32)
        part = part.astype(jnp.bfloat16)
        for t in range(4):
            p_v[c, t % 2, t // 2] = part[t * strip:(t + 1) * strip]
        c_copy(c).start()

    def stage2(c):
        c_copy(c).wait_recv()
        s2[c] = (p_v[c, core, 1 - yy].astype(jnp.float32)
                 + r1[c, 1 - yy].astype(jnp.float32)).astype(jnp.bfloat16)
        y_copy(c).start()

    def stage3(c):
        y_copy(c).wait_recv()
        o_ref[:, c * width:(c + 1) * width] = (
            p_v[c, core, yy].astype(jnp.float32) + r1[c, yy].astype(jnp.float32)
            + r2[c].astype(jnp.float32)).astype(jnp.bfloat16)

    def drain():
        for h, c in pieces:
            pl.when(has_up)(lambda: sent(along(me, h, c, -1)))
            pl.when(has_dn)(lambda: sent(along(me, h, c, 1)))
            sent(over_x(me, h, c))
        each(1, cz, lambda d: relay(d, sent, sent, False))

    lag2, lag3 = 2, 6
    for i in range(chunks + lag3):
        if i < chunks:
            stage1(i)
        if 0 <= i - lag2 < chunks:
            stage2(i - lag2)
        if i == chunks + lag2:
            drain()
        if 0 <= i - lag3 < chunks:
            stage3(i - lag3)

    for c in range(chunks):
        c_copy(c).wait_send()
        y_copy(c).wait_send()


def local_fn(nc, queries, keys, values, doc_blocks, block_order, out_weight):
    rows, qcols = queries.shape
    depth, cols = out_weight.shape
    heads_kv = keys.shape[1] // HEAD_SIZE
    chunks = 8
    width = cols // chunks
    strip = rows // 4
    bf, f32 = jnp.bfloat16, jnp.float32
    dma = pltpu.SemaphoreType.DMA
    hbm = pl.BlockSpec(memory_space=pltpu.HBM)
    long = nc // 2 > GROUP_BLOCKS
    operands = [pltpu.with_memory_space_constraint(a, pltpu.HBM) for a in (
        queries, keys, values, doc_blocks, block_order, out_weight)]
    return pl.pallas_call(
        functools.partial(kernel, nc, doc_blocks.shape[0], chunks, heads_kv),
        out_shape=jax.ShapeDtypeStruct((strip, cols), bf),
        in_specs=[hbm] * 6,
        out_specs=pl.BlockSpec(memory_space=pltpu.VMEM),
        scratch_shapes=[
            pltpu.SMEM(doc_blocks.shape, jnp.int32),
            pltpu.SMEM(block_order.shape, jnp.int32),
            pltpu.VMEM((chunks, depth, width), bf),
            pltpu.VMEM((rows, qcols), bf),
            pltpu.VMEM((rows, qcols), bf),
            pltpu.VMEM((chunks, 2, 2, strip, width), bf),
            pltpu.VMEM((chunks, 2, strip, width), bf),
            pltpu.VMEM((chunks, strip, width), bf),
            pltpu.VMEM((chunks, strip, width), bf),
            pltpu.VMEM((qcols if long else 8, HEAD_SIZE), f32),
            pltpu.VMEM((qcols if long else 8, 2 * HEAD_SIZE), f32),
            dma((2,)), dma((heads_kv, 2)), dma, dma((chunks,)),
            dma((nc, heads_kv, 2)), dma((nc, heads_kv, 2)), dma((nc, heads_kv, 2)),
            dma((nc, heads_kv, 2)),
            dma((chunks,)), dma((chunks,)), dma((chunks,)), dma((chunks,)),
        ] + [pltpu.VMEM((nc, BLOCK_TOKENS, HEAD_SIZE), bf)] * (2 * heads_kv),
        compiler_params=pltpu.CompilerParams(
            collective_id=0, has_side_effects=True, vmem_limit_bytes=48 * 2**20),
    )(*operands)


def solution(mesh):
    placed = (P("cp", "tp"), P("cp", "tp"), P("cp", "tp"), P(), P(), P("tp", None))
    assert mesh.shape["tp"] == 4
    return jax.shard_map(
        functools.partial(local_fn, mesh.shape["cp"]),
        mesh=mesh, in_specs=placed, out_specs=P(("cp", "tp"), None), check_vma=False,
    )
```
